128 devices in a mesh: outer: 16 (over y, x), span: 8 (over z, core).
Axes of the slice: x: 4, y: 4, z: 4, core: 2. Of those that a mesh axis runs over, the one named last changes fastest.
Arguments:
- queries_in: bfloat16 [32, 4096, 16, 128], P('outer', 'span'), may hold values from -6 to 6
- keys_in: bfloat16 [32, 4096, 16, 128], P('outer', 'span'), may hold values from -6 to 6
- values_in: bfloat16 [32, 4096, 16, 128], P('outer', 'span'), may hold values from -6 to 6
- gate_rows: bfloat16 [32, 4096, 16, 128], P('outer', 'span'), may hold values from -6 to 6
- out_weight: bfloat16 [2048, 2048], P('outer'), may hold values from -0.125 to 0.125
Outputs:
- mixer_out: bfloat16 [32, 4096, 2048], P('outer', 'span')
The draws below stay inside these ranges and needn't reach their ends.
All inputs are finite; a program needn't handle non-finite values.
Results may differ from the reference program's by a relative error of at most 0.0023.
Values may be sent and summed in bfloat16 or wider, within the bound.
No kernel may reach another device: no remote copies, remote signals or barrier semaphores. Data moves between devices by JAX's collectives and lax.ppermute only.
A program may use at most 256 MiB of HBM per device.

```python
import jax
import jax.numpy as jnp
from jax import lax

HEADS = 16
HEAD_SIZE = 128
BATCH = 32
TOKENS = 4096
WIDTH = 2048


def block_scale(own_key, dims, shards, low, largest):
    def one(position, parts):
        heights = jax.random.uniform(jax.random.fold_in(jax.random.fold_in(own_key, 6), position), (parts,), jnp.float32, low / len(shards), largest / len(shards))
        return jnp.repeat(jnp.exp(heights), dims[position] // parts).reshape((-1,) + (1,) * (len(dims) - position - 1))

    factor_of = one(*shards[0])
    for cut in shards[1:]:
        factor_of = factor_of * one(*cut)
    return factor_of


def scatter_about(own_key, dims, deviation, reach, shards=(), kind=jnp.bfloat16):
    entries = deviation * jax.random.normal(own_key, dims, jnp.float32)
    if shards:
        entries = entries * block_scale(own_key, dims, shards, -0.22, 0.18)
    return jnp.clip(entries, -reach, reach).astype(kind)


def setup_inputs(seed: int = 0) -> dict:
    streams_of = jax.random.split(jax.random.key(seed), 6)
    return {
        "queries_in": scatter_about(streams_of[0], (BATCH, TOKENS, HEADS, HEAD_SIZE), 1.0, 6.0, ((0, 16), (1, 8))),
        "keys_in": scatter_about(streams_of[1], (BATCH, TOKENS, HEADS, HEAD_SIZE), 1.0, 6.0, ((0, 16), (1, 8))),
        "values_in": scatter_about(streams_of[2], (BATCH, TOKENS, HEADS, HEAD_SIZE), 1.0, 6.0, ((0, 16), (1, 8))),
        "gate_rows": scatter_about(streams_of[3], (BATCH, TOKENS, HEADS, HEAD_SIZE), 1.0, 6.0, ((0, 16), (1, 8))),
        "out_weight": scatter_about(streams_of[4], (WIDTH, WIDTH), WIDTH ** -0.5, 0.125, ((0, 16),)),
    }


def feature_map(values):
    wide = values.astype(jnp.float32)
    return (jnp.where(wide > 0.0, wide + 1.0, jnp.exp(jnp.minimum(wide, 0.0)))).astype(jnp.bfloat16)


def close_heads(read, gate_rows, count):
    result = read * count ** 0.5
    result = result * jax.nn.sigmoid(gate_rows.astype(jnp.float32))
    return result.astype(jnp.bfloat16)


def ask_state(features, state, mass):
    small = lax.optimization_barrier(state.astype(jnp.bfloat16))
    top = jnp.einsum("bthd,bhde->bthe", features.astype(jnp.float32), small.astype(jnp.float32))
    bottom = jnp.einsum("bthd,bhd->bth", features.astype(jnp.float32), mass, precision=lax.Precision.HIGHEST)
    return top / (bottom + 1e-3)[..., None]


def reference(queries_in, keys_in, values_in, gate_rows, out_weight):
    query_feature, key_feature = lax.optimization_barrier((feature_map(queries_in), feature_map(keys_in)))
    state = jnp.einsum("bthd,bthe->bhde", key_feature.astype(jnp.float32), values_in.astype(jnp.float32)) / TOKENS
    mass = jnp.sum(key_feature.astype(jnp.float32), axis=1) / TOKENS
    mixed = close_heads(ask_state(query_feature, state, mass), gate_rows, TOKENS).reshape(BATCH, TOKENS, WIDTH)
    mixed = lax.optimization_barrier(mixed)
    mixer_out = jnp.einsum("btw,wv->btv", mixed.astype(jnp.float32), out_weight.astype(jnp.float32)).astype(jnp.bfloat16)
    return mixer_out
```

```python
import jax
import jax.numpy as jnp
from jax import lax
from jax.experimental import pallas as pl
from jax.experimental.pallas import tpu as pltpu
from jax.sharding import PartitionSpec as P


BF16, F16, F32 = jnp.bfloat16, jnp.float16, jnp.float32
SIDE = 4
AXES = ("outer", "span")
OFFSETS = (0, -1, 1, 2)


def device(y, x, z, core):
    return ((y % SIDE) * SIDE + x % SIDE) * 2 * SIDE + (z % SIDE) * 2 + core


def permute(value, target):
    pairs = []
    for y in range(SIDE):
        for x in range(SIDE):
            for z in range(SIDE):
                for core in range(2):
                    pairs.append((device(y, x, z, core), device(*target(y, x, z, core))))
    return lax.ppermute(value, AXES, pairs)


def to_partner(y, x, z, core):
    return y, x, z, 1 - core


def along_z(early):
    def target(y, x, z, core):
        if (core == 0) == early:
            return y, x, z ^ 1, core
        return y, x, 3 - z, core

    return target


def shifted(by, first):
    def target(y, x, z, core):
        if (core == 0) == first:
            return y, x + by, z, core
        return y + by, x, z, core

    return target


def feature(values):
    wide = values.astype(F32)
    return jnp.where(wide > 0.0, wide + 1.0, jnp.exp(jnp.minimum(wide, 0.0))).astype(BF16)


def params(mib, **more):
    return pltpu.CompilerParams(vmem_limit_bytes=mib << 20, **more)


def state_kernel(place, k_ref, v_ref, out_ref):
    step = pl.program_id(0)
    group = k_ref.shape[2]
    keys = pltpu.einshape("thd->htd", k_ref[0])
    values = pltpu.einshape("thd->htd", v_ref[0])
    rows = []
    for h in range(group):
        f = feature(keys[h])
        out_ref[step * group + h] = lax.dot_general(
            values[h], f, (((0,), (0,)), ((), ())), preferred_element_type=F32
        )
        rows.append(jnp.sum(f.astype(F32), axis=0, keepdims=True))
    last = out_ref.shape[0] - 1
    out_ref[last, pl.ds(pl.multiple_of(step * group, group), group), :] = jnp.concatenate(rows, axis=0)


def sequence(place, turn):
    return (place[1] & 1) ^ turn


def local_state(place, turn, keys, values):
    _, tokens, heads, size = keys.shape
    group = 8
    spec = pl.BlockSpec((1, tokens, group, size), lambda i, p: (sequence(p, turn), 0, i, 0))
    shape = (heads + 1, size, size)
    return pl.pallas_call(
        state_kernel,
        grid_spec=pltpu.PrefetchScalarGridSpec(
            num_scalar_prefetch=1,
            grid=(heads // group,),
            in_specs=[spec, spec],
            out_specs=pl.BlockSpec(shape, lambda i, p: (0, 0, 0)),
        ),
        out_shape=jax.ShapeDtypeStruct(shape, F32),
        compiler_params=params(24),
        cost_estimate=pl.CostEstimate(flops=4 * 10**9, bytes_accessed=5 << 20, transcendentals=0),
        name="local_state",
    )(place, keys, values)


def pack(state, mass, out_ref):
    heads = state.shape[0]
    out_ref[:heads] = state.astype(out_ref.dtype)
    high = mass.astype(BF16).astype(F32)
    out_ref[heads, : 2 * heads] = jnp.concatenate([high, mass - high], axis=0).astype(out_ref.dtype)


def first_kernel(a_ref, b_ref, total_ref, send_ref):
    heads = a_ref.shape[0] - 1
    total = (a_ref[...] + b_ref[...]) * 0.25
    total_ref[...] = total
    pack(total[:heads], total[heads, :heads], send_ref)


def next_kernel(a_ref, b_ref, *out_refs):
    heads = a_ref.shape[0] - 1
    state = a_ref[:heads] + b_ref[:heads]
    mass = a_ref[heads, :heads] + b_ref[heads, :heads] + b_ref[heads, heads : 2 * heads]
    if len(out_refs) > 1:
        out_refs[0][:heads] = state
        out_refs[0][heads, :heads] = mass
    pack(state, mass, out_refs[-1])


def join(kernel, a, b, types):
    vmem = pl.BlockSpec(memory_space=pltpu.VMEM)
    return pl.pallas_call(
        kernel,
        in_specs=[vmem, vmem],
        out_specs=[vmem] * len(types),
        out_shape=[jax.ShapeDtypeStruct(a.shape, t) for t in types],
        compiler_params=params(16),
        cost_estimate=pl.CostEstimate(flops=5 * 10**8, bytes_accessed=3 << 20, transcendentals=0),
    )(a, b)


def ready_kernel(place, q_ref, g_ref, f_ref, s_ref):
    block, heads, size = q_ref.shape[1:]
    at = pl.ds(pl.multiple_of(pl.program_id(0) * block, block), block)
    queries = pltpu.einshape("thd->htd", q_ref[0])
    gates = pltpu.einshape("thd->htd", g_ref[0])
    for h in range(heads):
        cut = slice(h * size, (h + 1) * size)
        f_ref[at, cut] = feature(queries[h])
        s_ref[at, cut] = 64.0 / (1.0 + jnp.exp(-gates[h].astype(F32)))


def ready(place, turn, queries, gates):
    _, tokens, heads, size = queries.shape
    block = 128
    spec = pl.BlockSpec((1, block, heads, size), lambda i, p: (sequence(p, turn), i, 0, 0))
    vmem = pl.BlockSpec(memory_space=pltpu.VMEM)
    shape = (tokens, heads * size)
    return pl.pallas_call(
        ready_kernel,
        grid_spec=pltpu.PrefetchScalarGridSpec(
            num_scalar_prefetch=1,
            grid=(tokens // block,),
            in_specs=[spec, spec],
            out_specs=[vmem, vmem],
        ),
        out_shape=[jax.ShapeDtypeStruct(shape, BF16), jax.ShapeDtypeStruct(shape, F32)],
        compiler_params=params(8),
        cost_estimate=pl.CostEstimate(flops=4 * 10**9, bytes_accessed=10 << 20, transcendentals=0),
        name="ready",
    )(place, queries, gates)


def head_at(place, n):
    y, x, core = place[0] >> 2, place[0] & 3, place[1] & 1
    second, first = OFFSETS[n // SIDE], OFFSETS[n % SIDE]
    down, across = jnp.where(core == 0, second, first), jnp.where(core == 0, first, second)
    return ((y + down) & 3) * SIDE + ((x + across) & 3)


def read_kernel(place, f_ref, s_ref, state_ref, mixed_ref, rhs):
    step = pl.program_id(0)
    heads = state_ref.shape[0] - 1
    size = state_ref.shape[-1]
    block = f_ref.shape[0] // pl.num_programs(0)

    @pl.when(step == 0)
    def _():
        for h in range(heads):
            rhs[h, :size, :size] = state_ref[h]
            rhs[h, :size, size:] = jnp.zeros((size, size), BF16)
            rhs[h, size:, :size] = jnp.broadcast_to(state_ref[heads, h : h + 1, :], (size, size))
            rhs[h, size:, size:] = jnp.broadcast_to(state_ref[heads, heads + h : heads + h + 1, :], (size, size))

    rows = pl.ds(pl.multiple_of(step * block, block), block)
    for n in range(heads):
        h = head_at(place, n)
        cut = pl.ds(pl.multiple_of(h * size, size), size)
        f = f_ref[rows, cut]
        both = lax.dot_general(
            jnp.concatenate([f, f], axis=1), rhs[h], (((1,), (1,)), ((), ())), preferred_element_type=F32
        )
        mixed_ref[rows, n * size : (n + 1) * size] = (both[:, :size] * s_ref[rows, cut] / (both[:, size:] + 1.024)).astype(BF16)


def read(place, features, scale, state):
    tokens, width = features.shape
    size = state.shape[-1]
    vmem = pl.BlockSpec(memory_space=pltpu.VMEM)
    return pl.pallas_call(
        read_kernel,
        grid_spec=pltpu.PrefetchScalarGridSpec(
            num_scalar_prefetch=1,
            grid=(2,),
            in_specs=[vmem] * 3,
            out_specs=vmem,
            scratch_shapes=[pltpu.VMEM((width // size, 2 * size, 2 * size), BF16)],
        ),
        out_shape=jax.ShapeDtypeStruct((tokens, width), BF16),
        compiler_params=params(8),
        cost_estimate=pl.CostEstimate(flops=3 * 10**9, bytes_accessed=8 << 20, transcendentals=0),
        name="read",
    )(place, features, scale, state)


def product(mixed_ref, rows, piece_refs, side):
    size = piece_refs[0].shape[1]
    total = None
    for p, piece in enumerate(piece_refs):
        slots = [p * SIDE + q if side == 0 else q * SIDE + p for q in range(SIDE)]
        left = jnp.concatenate([mixed_ref[rows, n * size : (n + 1) * size] for n in slots], axis=1)
        part = jnp.dot(left, piece[...].reshape(SIDE * size, -1), preferred_element_type=F32)
        total = part if total is None else total + part
    return total.astype(BF16)


def half_kernel(mixed_refs, piece_refs, out_ref):
    block = out_ref.shape[1] // pl.num_programs(0)
    rows = pl.ds(pl.multiple_of(pl.program_id(0) * block, block), block)
    for t, mixed in enumerate(mixed_refs):
        out_ref[t, rows, :] = product(mixed, rows, piece_refs, 0)


def first_half(mixed, pieces):
    vmem = pl.BlockSpec(memory_space=pltpu.VMEM)
    return pl.pallas_call(
        half_kernel,
        grid=(2,),
        in_specs=[[vmem] * 2, [vmem] * SIDE],
        out_specs=vmem,
        out_shape=jax.ShapeDtypeStruct((2, mixed[0].shape[0], pieces[0].shape[-1]), BF16),
        compiler_params=params(8),
        cost_estimate=pl.CostEstimate(flops=5 * 10**9, bytes_accessed=8 << 20, transcendentals=0),
        name="first_half",
    )(mixed, pieces)


def rest_kernel(place, mixed_refs, half_ref, piece_refs, out_ref):
    turn, step = pl.program_id(0), pl.program_id(1)
    block, half = out_ref.shape[1], half_ref.shape[-1]
    rows = pl.ds(pl.multiple_of(step * block, block), block)
    core = place[1] & 1

    def columns(side):
        return pl.ds(pl.multiple_of((core ^ side) * half, half), half)

    for t, mixed in enumerate(mixed_refs):

        @pl.when(turn == t)
        def _():
            out_ref[0, :, columns(0)] = half_ref[t, rows, :]
            out_ref[0, :, columns(1)] = product(mixed, rows, piece_refs, 1)


def rest(place, mixed, half, pieces):
    tokens, width = mixed[0].shape
    block = 256
    vmem = pl.BlockSpec(memory_space=pltpu.VMEM)
    return pl.pallas_call(
        rest_kernel,
        grid_spec=pltpu.PrefetchScalarGridSpec(
            num_scalar_prefetch=1,
            grid=(2, tokens // block),
            in_specs=[[vmem] * 2, vmem, [vmem] * SIDE],
            out_specs=pl.BlockSpec((1, block, width), lambda s, i, p: (sequence(p, s), i, 0)),
        ),
        out_shape=jax.ShapeDtypeStruct((2, tokens, width), BF16),
        compiler_params=params(12),
        cost_estimate=pl.CostEstimate(flops=5 * 10**9, bytes_accessed=10 << 20, transcendentals=0),
        name="rest",
    )(place, mixed, half, pieces)


def gather_weight(weight, core):
    half = weight.shape[1] // 2
    own = lax.dynamic_slice_in_dim(weight, core * half, half, axis=1)
    stack = jnp.stack([own] + [permute(own, shifted(by, True)) for by in (1, -1, 2)])
    return [stack] + [permute(stack, shifted(by, False)) for by in (1, -1, 2)]


def body(queries_in, keys_in, values_in, gate_rows, out_weight):
    outer, span = lax.axis_index("outer"), lax.axis_index("span")
    place = jnp.stack([outer, span]).astype(jnp.int32)
    queries_in, keys_in, values_in, gate_rows = (
        pltpu.with_memory_space_constraint(a, pltpu.HBM) for a in (queries_in, keys_in, values_in, gate_rows)
    )
    pieces = gather_weight(out_weight, span & 1)
    swapped = [permute(piece, to_partner) for piece in pieces]
    theirs = local_state(place, 1, keys_in, values_in)
    came = permute(theirs, to_partner)
    own = local_state(place, 0, keys_in, values_in)
    total, send = join(first_kernel, own, came, (F32, F32))
    came = permute(send.astype(F16), along_z(True)).astype(F32)
    total, send = join(next_kernel, total, came, (F32, F32))
    came = permute(send.astype(F16), along_z(False)).astype(F32)
    (done,) = join(next_kernel, total, came, (BF16,))
    other = permute(done, to_partner)
    mixed = []
    for turn, state in enumerate((done, other)):
        features, scale = ready(place, turn, queries_in, gate_rows)
        mixed.append(read(place, features, scale, state))
    half = first_half(mixed, pieces)
    return rest(place, mixed, half, swapped)


def solution(mesh):
    rows = P("outer", "span", None, None)
    return jax.shard_map(
        lambda *args: body(*args),
        mesh=mesh,
        in_specs=(rows, rows, rows, rows, P("outer", None)),
        out_specs=P("outer", "span", None),
        check_vma=False,
    )
```

```python
import functools

import jax
import jax.numpy as jnp
from jax import lax
from jax.experimental import pallas as pl
from jax.experimental.pallas import tpu as pltpu
from jax.sharding import PartitionSpec as P


BF16, F16, F32 = jnp.bfloat16, jnp.float16, jnp.float32
SIDE = 4
AXES = ("outer", "span")
OFFSETS = (0, -1, 1, 2)


def device(y, x, z, core):
    return ((y % SIDE) * SIDE + x % SIDE) * 2 * SIDE + (z % SIDE) * 2 + core


def permute(value, target):
    pairs = []
    for y in range(SIDE):
        for x in range(SIDE):
            for z in range(SIDE):
                for core in range(2):
                    pairs.append((device(y, x, z, core), device(*target(y, x, z, core))))
    return lax.ppermute(value, AXES, pairs)


def to_partner(y, x, z, core):
    return y, x, z, 1 - core


def along_z(early):
    def target(y, x, z, core):
        if (core == 0) == early:
            return y, x, z ^ 1, core
        return y, x, 3 - z, core

    return target


def shifted(by, first):
    def target(y, x, z, core):
        if (core == 0) == first:
            return y, x + by, z, core
        return y + by, x, z, core

    return target


def feature(values):
    wide = values.astype(F32)
    return jnp.where(wide > 0.0, wide + 1.0, jnp.exp(jnp.minimum(wide, 0.0))).astype(BF16)


def params(mib, **more):
    return pltpu.CompilerParams(vmem_limit_bytes=mib << 20, **more)


def sequence(place, turn):
    return (place[1] & 1) ^ turn


def state_kernel(turn, place, k_ref, v_ref, out_ref):
    heads = k_ref.shape[2]
    group = 8
    at = sequence(place, turn)
    for first in range(0, heads, group):
        keys = pltpu.einshape("thd->htd", k_ref[at, :, first : first + group, :])
        values = pltpu.einshape("thd->htd", v_ref[at, :, first : first + group, :])
        rows = []
        for h in range(group):
            f = feature(keys[h])
            out_ref[first + h] = lax.dot_general(values[h], f, (((0,), (0,)), ((), ())), preferred_element_type=F32)
            rows.append(jnp.sum(f.astype(F32), axis=0, keepdims=True))
        out_ref[heads, first : first + group, :] = jnp.concatenate(rows, axis=0)


def local_state(place, turn, keys, values):
    heads, size = keys.shape[2:]
    vmem = pl.BlockSpec(memory_space=pltpu.VMEM)
    return pl.pallas_call(
        functools.partial(state_kernel, turn),
        in_specs=[pl.BlockSpec(memory_space=pltpu.SMEM), vmem, vmem],
        out_specs=vmem,
        out_shape=jax.ShapeDtypeStruct((heads + 1, size, size), F32),
        compiler_params=params(16),
        cost_estimate=pl.CostEstimate(flops=4 * 10**9, bytes_accessed=5 << 20, transcendentals=0),
        name="local_state",
    )(place, keys, values)


def pack(state, mass, out_ref):
    heads = state.shape[0]
    out_ref[:heads] = state.astype(out_ref.dtype)
    high = mass.astype(BF16).astype(F32)
    out_ref[heads, : 2 * heads] = jnp.concatenate([high, mass - high], axis=0).astype(out_ref.dtype)


def first_kernel(a_ref, b_ref, total_ref, send_ref):
    heads = a_ref.shape[0] - 1
    total = (a_ref[...] + b_ref[...]) * 0.25
    total_ref[...] = total
    pack(total[:heads], total[heads, :heads], send_ref)


def next_kernel(a_ref, b_ref, *out_refs):
    heads = a_ref.shape[0] - 1
    state = a_ref[:heads] + b_ref[:heads]
    mass = a_ref[heads, :heads] + b_ref[heads, :heads] + b_ref[heads, heads : 2 * heads]
    if len(out_refs) > 1:
        out_refs[0][:heads] = state
        out_refs[0][heads, :heads] = mass
    pack(state, mass, out_refs[-1])


def join(kernel, a, b, types):
    vmem = pl.BlockSpec(memory_space=pltpu.VMEM)
    return pl.pallas_call(
        kernel,
        in_specs=[vmem, vmem],
        out_specs=[vmem] * len(types),
        out_shape=[jax.ShapeDtypeStruct(a.shape, t) for t in types],
        compiler_params=params(16),
        cost_estimate=pl.CostEstimate(flops=5 * 10**8, bytes_accessed=3 << 20, transcendentals=0),
    )(a, b)


def ready_kernel(turn, place, q_ref, g_ref, f_ref, s_ref):
    heads, size = q_ref.shape[2:]
    block = f_ref.shape[0] // pl.num_programs(0)
    at = pl.ds(pl.multiple_of(pl.program_id(0) * block, block), block)
    which = sequence(place, turn)
    queries = pltpu.einshape("thd->htd", q_ref[which, at, :, :])
    gates = pltpu.einshape("thd->htd", g_ref[which, at, :, :])
    for h in range(heads):
        cut = slice(h * size, (h + 1) * size)
        f_ref[at, cut] = feature(queries[h])
        s_ref[at, cut] = 1.0 + jnp.exp(-gates[h].astype(F32))


def ready(place, turn, queries, gates):
    _, tokens, heads, size = queries.shape
    vmem = pl.BlockSpec(memory_space=pltpu.VMEM)
    shape = (tokens, heads * size)
    return pl.pallas_call(
        functools.partial(ready_kernel, turn),
        grid=(4,),
        in_specs=[pl.BlockSpec(memory_space=pltpu.SMEM), vmem, vmem],
        out_specs=[vmem, vmem],
        out_shape=[jax.ShapeDtypeStruct(shape, BF16), jax.ShapeDtypeStruct(shape, F32)],
        compiler_params=params(8),
        cost_estimate=pl.CostEstimate(flops=4 * 10**9, bytes_accessed=10 << 20, transcendentals=0),
        name="ready",
    )(place, queries, gates)


def head_at(place, n):
    y, x, core = place[0] >> 2, place[0] & 3, place[1] & 1
    second, first = OFFSETS[n // SIDE], OFFSETS[n % SIDE]
    down, across = jnp.where(core == 0, second, first), jnp.where(core == 0, first, second)
    return ((y + down) & 3) * SIDE + ((x + across) & 3)


def read_kernel(place, f_ref, s_ref, state_ref, mixed_ref, rhs):
    step = pl.program_id(0)
    heads = state_ref.shape[0] - 1
    size = state_ref.shape[-1]
    block = f_ref.shape[0] // pl.num_programs(0)

    @pl.when(step == 0)
    def _():
        for h in range(heads):
            rhs[h, :size, :size] = state_ref[h]
            rhs[h, :size, size:] = jnp.zeros((size, size), BF16)
            rhs[h, size:, :size] = jnp.broadcast_to(state_ref[heads, h : h + 1, :], (size, size))
            rhs[h, size:, size:] = jnp.broadcast_to(state_ref[heads, heads + h : heads + h + 1, :], (size, size))

    rows = pl.ds(pl.multiple_of(step * block, block), block)
    for n in range(heads):
        h = head_at(place, n)
        cut = pl.ds(pl.multiple_of(h * size, size), size)
        f = f_ref[rows, cut]
        both = lax.dot_general(
            jnp.concatenate([f, f], axis=1), rhs[h], (((1,), (1,)), ((), ())), preferred_element_type=F32
        )
        mixed_ref[rows, n * size : (n + 1) * size] = (both[:, :size] * (64.0 / ((both[:, size:] + 1.024) * s_ref[rows, cut]))).astype(BF16)


def read(place, features, scale, state):
    tokens, width = features.shape
    size = state.shape[-1]
    vmem = pl.BlockSpec(memory_space=pltpu.VMEM)
    return pl.pallas_call(
        read_kernel,
        grid_spec=pltpu.PrefetchScalarGridSpec(
            num_scalar_prefetch=1,
            grid=(2,),
            in_specs=[vmem] * 3,
            out_specs=vmem,
            scratch_shapes=[pltpu.VMEM((width // size, 2 * size, 2 * size), BF16)],
        ),
        out_shape=jax.ShapeDtypeStruct((tokens, width), BF16),
        compiler_params=params(8),
        cost_estimate=pl.CostEstimate(flops=3 * 10**9, bytes_accessed=8 << 20, transcendentals=0),
        name="read",
    )(place, features, scale, state)


def product(mixed_ref, rows, piece_refs, side):
    size = piece_refs[0].shape[1]
    total = None
    for p, piece in enumerate(piece_refs):
        slots = [p * SIDE + q if side == 0 else q * SIDE + p for q in range(SIDE)]
        left = jnp.concatenate([mixed_ref[rows, n * size : (n + 1) * size] for n in slots], axis=1)
        part = jnp.dot(left, piece[...].reshape(SIDE * size, -1), preferred_element_type=F32)
        total = part if total is None else total + part
    return total.astype(BF16)


def first_half_kernel(mixed_refs, piece_refs, out_ref):
    block = out_ref.shape[1] // pl.num_programs(0)
    rows = pl.ds(pl.multiple_of(pl.program_id(0) * block, block), block)
    for t, mixed in enumerate(mixed_refs):
        out_ref[t, rows, :] = product(mixed, rows, piece_refs, 0)


def first_half(mixed, pieces):
    vmem = pl.BlockSpec(memory_space=pltpu.VMEM)
    return pl.pallas_call(
        first_half_kernel,
        grid=(2,),
        in_specs=[[vmem] * 2, [vmem] * SIDE],
        out_specs=vmem,
        out_shape=jax.ShapeDtypeStruct((2, mixed[0].shape[0], pieces[0].shape[-1]), BF16),
        compiler_params=params(8),
        cost_estimate=pl.CostEstimate(flops=5 * 10**9, bytes_accessed=8 << 20, transcendentals=0),
        name="first_half",
    )(mixed, pieces)


def last_half_kernel(place, mixed_refs, half_ref, piece_refs, out_ref, held, sems, half_sems):
    cuts, block, half = held.shape
    per = cuts // 2

    def columns(side):
        return pl.ds(pl.multiple_of(sequence(place, side) * half, half), half)

    copies = []
    for t in range(2):
        copies.append(pltpu.make_async_copy(half_ref.at[t], out_ref.at[sequence(place, t), :, columns(0)], half_sems.at[t]))
        copies[-1].start()
    for t, mixed in enumerate(mixed_refs):
        for i in range(per):
            n = t * per + i
            held[n] = product(mixed, slice(i * block, (i + 1) * block), piece_refs, 1)
            target = out_ref.at[sequence(place, t), pl.ds(i * block, block), columns(1)]
            copies.append(pltpu.make_async_copy(held.at[n], target, sems.at[n]))
            copies[-1].start()
    for copy in copies:
        copy.wait()


def last_half(place, mixed, half, pieces):
    tokens, width = mixed[0].shape
    block = 256
    vmem = pl.BlockSpec(memory_space=pltpu.VMEM)
    cuts = 2 * tokens // block
    return pl.pallas_call(
        last_half_kernel,
        in_specs=[pl.BlockSpec(memory_space=pltpu.SMEM), [vmem] * 2, vmem, [vmem] * SIDE],
        out_specs=pl.BlockSpec(memory_space=pltpu.HBM),
        out_shape=jax.ShapeDtypeStruct((2, tokens, width), BF16),
        scratch_shapes=[
            pltpu.VMEM((cuts, block, width // 2), BF16),
            pltpu.SemaphoreType.DMA((cuts,)),
            pltpu.SemaphoreType.DMA((2,)),
        ],
        compiler_params=params(10),
        cost_estimate=pl.CostEstimate(flops=5 * 10**9, bytes_accessed=8 << 20, transcendentals=0),
        name="last_half",
    )(place, mixed, half, pieces)


def take_kernel(place, w_ref, out_ref, sem):
    half = out_ref.shape[1]
    columns = pl.ds(pl.multiple_of(sequence(place, 0) * half, half), half)
    copy = pltpu.make_async_copy(w_ref.at[:, columns], out_ref, sem)
    copy.start()
    copy.wait()


def own_columns(place, weight):
    rows, width = weight.shape
    return pl.pallas_call(
        take_kernel,
        in_specs=[pl.BlockSpec(memory_space=pltpu.SMEM), pl.BlockSpec(memory_space=pltpu.HBM)],
        out_specs=pl.BlockSpec(memory_space=pltpu.VMEM),
        out_shape=jax.ShapeDtypeStruct((rows, width // 2), weight.dtype),
        scratch_shapes=[pltpu.SemaphoreType.DMA],
        compiler_params=params(4),
        cost_estimate=pl.CostEstimate(flops=6 * 10**9, bytes_accessed=1 << 20, transcendentals=0),
        name="own_columns",
    )(place, weight)


def gather_weight(place, weight):
    own = own_columns(place, weight)
    stack = jnp.stack([own] + [permute(own, shifted(by, True)) for by in (1, -1, 2)])
    return [stack] + [permute(stack, shifted(by, False)) for by in (1, -1, 2)]


def body(queries_in, keys_in, values_in, gate_rows, out_weight):
    outer, span = lax.axis_index("outer"), lax.axis_index("span")
    place = jnp.stack([outer, span]).astype(jnp.int32)
    out_weight = pltpu.with_memory_space_constraint(out_weight, pltpu.HBM)
    pieces = gather_weight(place, out_weight)
    swapped = [permute(piece, to_partner) for piece in pieces]
    theirs = local_state(place, 1, keys_in, values_in)
    came = permute(theirs, to_partner)
    own = local_state(place, 0, keys_in, values_in)
    total, send = join(first_kernel, own, came, (F32, F32))
    came = permute(send.astype(F16), along_z(True)).astype(F32)
    total, send = join(next_kernel, total, came, (F32, F32))
    came = permute(send.astype(F16), along_z(False)).astype(F32)
    (done,) = join(next_kernel, total, came, (BF16,))
    other = permute(done, to_partner)
    mixed = []
    for turn, state in enumerate((done, other)):
        features, scale = ready(place, turn, queries_in, gate_rows)
        mixed.append(read(place, features, scale, state))
    out = first_half(mixed, pieces)
    return last_half(place, mixed, out, swapped)


def solution(mesh):
    rows = P("outer", "span", None, None)
    return jax.shard_map(
        lambda *args: body(*args),
        mesh=mesh,
        in_specs=(rows, rows, rows, rows, P("outer", None)),
        out_specs=P("outer", "span", None),
        check_vma=False,
    )
```

```python
import functools

import jax
import jax.numpy as jnp
from jax import lax
from jax.experimental import pallas as pl
from jax.experimental.pallas import tpu as pltpu
from jax.sharding import PartitionSpec as P


BF16, F16, F32 = jnp.bfloat16, jnp.float16, jnp.float32
SIDE = 4
AXES = ("outer", "span")
OFFSETS = (0, -1, 1, 2)


def device(y, x, z, core):
    return ((y % SIDE) * SIDE + x % SIDE) * 2 * SIDE + (z % SIDE) * 2 + core


def permute(value, target):
    pairs = []
    for y in range(SIDE):
        for x in range(SIDE):
            for z in range(SIDE):
                for core in range(2):
                    pairs.append((device(y, x, z, core), device(*target(y, x, z, core))))
    return lax.ppermute(value, AXES, pairs)


def to_partner(y, x, z, core):
    return y, x, z, 1 - core


def along_z(early):
    def target(y, x, z, core):
        if (core == 0) == early:
            return y, x, z ^ 1, core
        return y, x, 3 - z, core

    return target


def shifted(by, first):
    def target(y, x, z, core):
        if (core == 0) == first:
            return y, x + by, z, core
        return y + by, x, z, core

    return target


def feature(values):
    grown = jnp.exp(values.astype(F32)).astype(BF16)
    return jnp.where(values > 0, values + jnp.ones((), BF16), grown)


def params(mib, **more):
    return pltpu.CompilerParams(vmem_limit_bytes=mib << 20, **more)


def sequence(place, turn):
    return (place[1] & 1) ^ turn


def state_kernel(turn, place, k_ref, v_ref, out_ref):
    tokens, heads, size = k_ref.shape[1:]
    at = sequence(place, turn)
    keys = pltpu.einshape("thd->htd", k_ref[at])
    values = pltpu.einshape("thd->htd", v_ref[at])
    ones = jnp.ones((8, tokens), BF16)
    rows = []
    for h in range(0, heads, 2):
        f = jnp.concatenate([feature(keys[h]), feature(keys[h + 1])], axis=1)
        v = jnp.concatenate([values[h], values[h + 1]], axis=1)
        both = lax.dot_general(v, f, (((0,), (0,)), ((), ())), preferred_element_type=F32)
        out_ref[h] = both[:size, :size]
        out_ref[h + 1] = both[size:, size:]
        mass = jnp.dot(ones, f, preferred_element_type=F32)[:1]
        rows += [mass[:, :size], mass[:, size:]]
    out_ref[heads, :heads, :] = jnp.concatenate(rows, axis=0)


def local_state(place, turn, keys, values):
    heads, size = keys.shape[2:]
    vmem = pl.BlockSpec(memory_space=pltpu.VMEM)
    return pl.pallas_call(
        functools.partial(state_kernel, turn),
        in_specs=[pl.BlockSpec(memory_space=pltpu.SMEM), vmem, vmem],
        out_specs=vmem,
        out_shape=jax.ShapeDtypeStruct((heads + 1, size, size), F32),
        compiler_params=params(16),
        cost_estimate=pl.CostEstimate(flops=4 * 10**9, bytes_accessed=5 << 20, transcendentals=0),
        name="local_state",
    )(place, keys, values)


def pack(state, mass, out_ref):
    heads = state.shape[0]
    out_ref[:heads] = state.astype(out_ref.dtype)
    high = mass.astype(BF16).astype(F32)
    out_ref[heads, : 2 * heads] = jnp.concatenate([high, mass - high], axis=0).astype(out_ref.dtype)


def first_kernel(a_ref, b_ref, total_ref, send_ref):
    heads = a_ref.shape[0] - 1
    total = (a_ref[...] + b_ref[...]) * 0.25
    total_ref[...] = total
    pack(total[:heads], total[heads, :heads], send_ref)


def next_kernel(a_ref, b_ref, *out_refs):
    heads = a_ref.shape[0] - 1
    state = a_ref[:heads] + b_ref[:heads]
    mass = a_ref[heads, :heads] + b_ref[heads, :heads] + b_ref[heads, heads : 2 * heads]
    if len(out_refs) > 1:
        out_refs[0][:heads] = state
        out_refs[0][heads, :heads] = mass
    pack(state, mass, out_refs[-1])


def join(kernel, a, b, types):
    vmem = pl.BlockSpec(memory_space=pltpu.VMEM)
    return pl.pallas_call(
        kernel,
        in_specs=[vmem, vmem],
        out_specs=[vmem] * len(types),
        out_shape=[jax.ShapeDtypeStruct(a.shape, t) for t in types],
        compiler_params=params(16),
        cost_estimate=pl.CostEstimate(flops=5 * 10**8, bytes_accessed=3 << 20, transcendentals=0),
    )(a, b)


def ready_kernel(turn, place, q_ref, g_ref, f_ref, s_ref):
    heads, size = q_ref.shape[2:]
    which = sequence(place, turn)
    queries = pltpu.einshape("thd->htd", q_ref[which])
    gates = pltpu.einshape("thd->htd", g_ref[which])
    for h in range(heads):
        cut = slice(h * size, (h + 1) * size)
        f_ref[:, cut] = feature(queries[h])
        s_ref[:, cut] = 1.0 + jnp.exp(-gates[h].astype(F32))


def ready(place, turn, queries, gates):
    _, tokens, heads, size = queries.shape
    vmem = pl.BlockSpec(memory_space=pltpu.VMEM)
    shape = (tokens, heads * size)
    return pl.pallas_call(
        functools.partial(ready_kernel, turn),
        in_specs=[pl.BlockSpec(memory_space=pltpu.SMEM), vmem, vmem],
        out_specs=[vmem, vmem],
        out_shape=[jax.ShapeDtypeStruct(shape, BF16), jax.ShapeDtypeStruct(shape, F32)],
        compiler_params=params(8),
        cost_estimate=pl.CostEstimate(flops=4 * 10**9, bytes_accessed=10 << 20, transcendentals=0),
        name="ready",
    )(place, queries, gates)


def head_at(place, n):
    y, x, core = place[0] >> 2, place[0] & 3, place[1] & 1
    second, first = OFFSETS[n // SIDE], OFFSETS[n % SIDE]
    down, across = jnp.where(core == 0, second, first), jnp.where(core == 0, first, second)
    return ((y + down) & 3) * SIDE + ((x + across) & 3)


def read_kernel(place, f_ref, s_ref, state_ref, mixed_ref, rhs):
    heads = state_ref.shape[0] - 1
    size = state_ref.shape[-1]
    for h in range(heads):
        rhs[h, :size, :size] = state_ref[h]
        rhs[h, :size, size:] = jnp.zeros((size, size), BF16)
        rhs[h, size:, :size] = jnp.broadcast_to(state_ref[heads, h : h + 1, :], (size, size))
        rhs[h, size:, size:] = jnp.broadcast_to(state_ref[heads, heads + h : heads + h + 1, :], (size, size))
    for n in range(heads):
        h = head_at(place, n)
        cut = pl.ds(pl.multiple_of(h * size, size), size)
        f = f_ref[:, cut]
        both = lax.dot_general(
            jnp.concatenate([f, f], axis=1), rhs[h], (((1,), (1,)), ((), ())), preferred_element_type=F32
        )
        scale = 64.0 / ((both[:, size:] + 1.024) * s_ref[:, cut])
        mixed_ref[:, n * size : (n + 1) * size] = (both[:, :size] * scale).astype(BF16)


def read(place, features, scale, state):
    tokens, width = features.shape
    size = state.shape[-1]
    vmem = pl.BlockSpec(memory_space=pltpu.VMEM)
    return pl.pallas_call(
        read_kernel,
        in_specs=[pl.BlockSpec(memory_space=pltpu.SMEM)] + [vmem] * 3,
        out_specs=vmem,
        out_shape=jax.ShapeDtypeStruct((tokens, width), BF16),
        scratch_shapes=[pltpu.VMEM((width // size, 2 * size, 2 * size), BF16)],
        compiler_params=params(8),
        cost_estimate=pl.CostEstimate(flops=3 * 10**9, bytes_accessed=8 << 20, transcendentals=0),
        name="read",
    )(place, features, scale, state)


def product(mixed_ref, rows, piece_refs, side, total=None):
    size = piece_refs[0][1].shape[1]
    for p, piece in piece_refs:
        slots = [p * SIDE + q if side == 0 else q * SIDE + p for q in range(SIDE)]
        left = jnp.concatenate([mixed_ref[rows, n * size : (n + 1) * size] for n in slots], axis=1)
        part = jnp.dot(left, piece[...].reshape(SIDE * size, -1), preferred_element_type=F32)
        total = part if total is None else total + part
    return total


def open_kernel(numbers, mixed_refs, piece_refs, out_ref):
    block = out_ref.shape[2] // pl.num_programs(0)
    rows = pl.ds(pl.multiple_of(pl.program_id(0) * block, block), block)
    for side in range(2):
        some = [(p, piece_refs[0][i] if side == 0 else piece_refs[1].at[i]) for i, p in enumerate(numbers)]
        for t, mixed in enumerate(mixed_refs):
            out_ref[side, t, rows, :] = product(mixed, rows, some, side)


def open_products(mixed, numbers, pieces):
    vmem = pl.BlockSpec(memory_space=pltpu.VMEM)
    return pl.pallas_call(
        functools.partial(open_kernel, numbers),
        grid=(2,),
        in_specs=[[vmem] * 2, [[vmem] * len(numbers), vmem]],
        out_specs=vmem,
        out_shape=jax.ShapeDtypeStruct((2, 2, mixed[0].shape[0], pieces[0][0].shape[-1]), F32),
        compiler_params=params(10),
        cost_estimate=pl.CostEstimate(flops=5 * 10**9, bytes_accessed=8 << 20, transcendentals=0),
        name="open_products",
    )(mixed, pieces)


def own_kernel(numbers, mixed_refs, open_ref, piece_refs, out_ref):
    block = out_ref.shape[1] // 2
    for t, mixed in enumerate(mixed_refs):
        for i in range(2):
            rows = slice(i * block, (i + 1) * block)
            some = list(zip(numbers, piece_refs))
            out_ref[t, rows, :] = product(mixed, rows, some, 0, open_ref[0, t, rows, :]).astype(BF16)


def own_half(mixed, opened, numbers, pieces):
    vmem = pl.BlockSpec(memory_space=pltpu.VMEM)
    return pl.pallas_call(
        functools.partial(own_kernel, numbers),
        in_specs=[[vmem] * 2, vmem, [vmem] * len(numbers)],
        out_specs=vmem,
        out_shape=jax.ShapeDtypeStruct(opened.shape[1:], BF16),
        compiler_params=params(8),
        cost_estimate=pl.CostEstimate(flops=3 * 10**9, bytes_accessed=8 << 20, transcendentals=0),
        name="own_half",
    )(mixed, opened, pieces)


def last_kernel(numbers, place, mixed_refs, open_ref, half_ref, piece_refs, out_ref, held, sems, half_sems):
    cuts, block, half = held.shape
    per = cuts // 2

    def columns(side):
        return pl.ds(pl.multiple_of(sequence(place, side) * half, half), half)

    copies = []
    for t in range(2):
        copies.append(pltpu.make_async_copy(half_ref.at[t], out_ref.at[sequence(place, t), :, columns(0)], half_sems.at[t]))
        copies[-1].start()
    for t, mixed in enumerate(mixed_refs):
        for i in range(per):
            n = t * per + i
            rows = slice(i * block, (i + 1) * block)
            some = [(p, piece_refs.at[j]) for j, p in enumerate(numbers)]
            held[n] = product(mixed, rows, some, 1, open_ref[1, t, rows, :]).astype(BF16)
            target = out_ref.at[sequence(place, t), pl.ds(i * block, block), columns(1)]
            copies.append(pltpu.make_async_copy(held.at[n], target, sems.at[n]))
            copies[-1].start()
    for copy in copies:
        copy.wait()


def last_half(place, mixed, opened, half, numbers, pieces):
    tokens, width = mixed[0].shape
    block = 256
    vmem = pl.BlockSpec(memory_space=pltpu.VMEM)
    cuts = 2 * tokens // block
    return pl.pallas_call(
        functools.partial(last_kernel, numbers),
        in_specs=[pl.BlockSpec(memory_space=pltpu.SMEM), [vmem] * 2, vmem, vmem, vmem],
        out_specs=pl.BlockSpec(memory_space=pltpu.HBM),
        out_shape=jax.ShapeDtypeStruct((2, tokens, width), BF16),
        scratch_shapes=[
            pltpu.VMEM((cuts, block, width // 2), BF16),
            pltpu.SemaphoreType.DMA((cuts,)),
            pltpu.SemaphoreType.DMA((2,)),
        ],
        compiler_params=params(10),
        cost_estimate=pl.CostEstimate(flops=3 * 10**9, bytes_accessed=8 << 20, transcendentals=0),
        name="last_half",
    )(place, mixed, opened, half, pieces)


def take_kernel(place, w_ref, out_ref, sem):
    half = out_ref.shape[1]
    columns = pl.ds(pl.multiple_of(sequence(place, 0) * half, half), half)
    copy = pltpu.make_async_copy(w_ref.at[:, columns], out_ref, sem)
    copy.start()
    copy.wait()


def own_columns(place, weight):
    rows, width = weight.shape
    return pl.pallas_call(
        take_kernel,
        in_specs=[pl.BlockSpec(memory_space=pltpu.SMEM), pl.BlockSpec(memory_space=pltpu.HBM)],
        out_specs=pl.BlockSpec(memory_space=pltpu.VMEM),
        out_shape=jax.ShapeDtypeStruct((rows, width // 2), weight.dtype),
        scratch_shapes=[pltpu.SemaphoreType.DMA],
        compiler_params=params(4),
        cost_estimate=pl.CostEstimate(flops=6 * 10**9, bytes_accessed=1 << 20, transcendentals=0),
        name="own_columns",
    )(place, weight)


def body(queries_in, keys_in, values_in, gate_rows, out_weight):
    outer, span = lax.axis_index("outer"), lax.axis_index("span")
    place = jnp.stack([outer, span]).astype(jnp.int32)
    own = own_columns(place, pltpu.with_memory_space_constraint(out_weight, pltpu.HBM))

    near = [permute(own, shifted(by, True)) for by in (1, -1, 2)]
    stack = jnp.stack([own] + near)
    stacks = [stack] + [permute(stack, shifted(by, False)) for by in (1, -1, 2)]
    early, late = (0, 3), (1, 2)
    pieces = []
    for numbers in (early, late):
        held = [stacks[p] for p in numbers]
        swapped = permute(jnp.stack(held), to_partner)
        pieces.append([held, swapped])

    theirs = local_state(place, 1, keys_in, values_in)
    came = permute(theirs, to_partner)
    own = local_state(place, 0, keys_in, values_in)
    total, send = join(first_kernel, own, came, (F32, F32))
    came = permute(send.astype(F16), along_z(True)).astype(F32)
    total, send = join(next_kernel, total, came, (F32, F32))
    came = permute(send.astype(F16), along_z(False)).astype(F32)
    (done,) = join(next_kernel, total, came, (BF16,))
    other = permute(done, to_partner)
    mixed = []
    for turn, state in enumerate((done, other)):
        features, scale = ready(place, turn, queries_in, gate_rows)
        mixed.append(read(place, features, scale, state))
    opened = open_products(mixed, early, pieces[0])
    half = own_half(mixed, opened, late, pieces[1][0])
    return last_half(place, mixed, opened, half, late, pieces[1][1])


def solution(mesh):
    rows = P("outer", "span", None, None)
    return jax.shard_map(
        lambda *args: body(*args),
        mesh=mesh,
        in_specs=(rows, rows, rows, rows, P("outer", None)),
        out_specs=P("outer", "span", None),
        check_vma=False,
    )
```

```python
import functools

import jax
import jax.numpy as jnp
from jax import lax
from jax.experimental import pallas as pl
from jax.experimental.pallas import tpu as pltpu
from jax.sharding import PartitionSpec as P


BF16, F16, F32 = jnp.bfloat16, jnp.float16, jnp.float32
SIDE = 4
AXES = ("outer", "span")
OFFSETS = (0, -1, 1, 2)


def device(y, x, z, core):
    return ((y % SIDE) * SIDE + x % SIDE) * 2 * SIDE + (z % SIDE) * 2 + core


def permute(value, target):
    pairs = []
    for y in range(SIDE):
        for x in range(SIDE):
            for z in range(SIDE):
                for core in range(2):
                    pairs.append((device(y, x, z, core), device(*target(y, x, z, core))))
    return lax.ppermute(value, AXES, pairs)


def to_partner(y, x, z, core):
    return y, x, z, 1 - core


def along_z(early):
    def target(y, x, z, core):
        if (core == 0) == early:
            return y, x, z ^ 1, core
        return y, x, 3 - z, core

    return target


def shifted(by, first):
    def target(y, x, z, core):
        if (core == 0) == first:
            return y, x + by, z, core
        return y + by, x, z, core

    return target


def feature(values):
    grown = jnp.exp(values.astype(F32)).astype(BF16)
    return jnp.where(values > 0, values + jnp.ones((), BF16), grown)


def params(mib, **more):
    return pltpu.CompilerParams(vmem_limit_bytes=mib << 20, **more)


def sequence(place, turn):
    return (place[1] & 1) ^ turn


def state_kernel(turn, place, k_ref, v_ref, out_ref):
    tokens, heads, size = k_ref.shape[1:]
    at = sequence(place, turn)
    keys = pltpu.einshape("thd->htd", k_ref[at])
    values = pltpu.einshape("thd->htd", v_ref[at])
    ones = jnp.ones((8, tokens), BF16)
    rows = []
    for h in range(0, heads, 2):
        f = jnp.concatenate([feature(keys[h]), feature(keys[h + 1])], axis=1)
        v = jnp.concatenate([values[h], values[h + 1]], axis=1)
        both = lax.dot_general(v, f, (((0,), (0,)), ((), ())), preferred_element_type=F32)
        out_ref[h] = both[:size, :size]
        out_ref[h + 1] = both[size:, size:]
        mass = jnp.dot(ones, f, preferred_element_type=F32)[:1]
        rows += [mass[:, :size], mass[:, size:]]
    out_ref[heads, :heads, :] = jnp.concatenate(rows, axis=0)


def local_state(place, turn, keys, values):
    heads, size = keys.shape[2:]
    vmem = pl.BlockSpec(memory_space=pltpu.VMEM)
    return pl.pallas_call(
        functools.partial(state_kernel, turn),
        in_specs=[pl.BlockSpec(memory_space=pltpu.SMEM), vmem, vmem],
        out_specs=vmem,
        out_shape=jax.ShapeDtypeStruct((heads + 1, size, size), F32),
        compiler_params=params(16),
        cost_estimate=pl.CostEstimate(flops=4 * 10**9, bytes_accessed=5 << 20, transcendentals=0),
        name="local_state",
    )(place, keys, values)


def pack(state, mass, out_ref):
    heads = state.shape[0]
    out_ref[:heads] = state.astype(out_ref.dtype)
    high = mass.astype(BF16).astype(F32)
    out_ref[heads, : 2 * heads] = jnp.concatenate([high, mass - high], axis=0).astype(out_ref.dtype)


def first_kernel(a_ref, b_ref, total_ref, send_ref):
    heads = a_ref.shape[0] - 1
    total = (a_ref[...] + b_ref[...]) * 0.25
    total_ref[...] = total
    pack(total[:heads], total[heads, :heads], send_ref)


def next_kernel(a_ref, b_ref, *out_refs):
    heads = a_ref.shape[0] - 1
    state = a_ref[:heads] + b_ref[:heads]
    mass = a_ref[heads, :heads] + b_ref[heads, :heads] + b_ref[heads, heads : 2 * heads]
    if len(out_refs) > 1:
        out_refs[0][:heads] = state
        out_refs[0][heads, :heads] = mass
    pack(state, mass, out_refs[-1])


def join(kernel, a, b, types):
    vmem = pl.BlockSpec(memory_space=pltpu.VMEM)
    return pl.pallas_call(
        kernel,
        in_specs=[vmem, vmem],
        out_specs=[vmem] * len(types),
        out_shape=[jax.ShapeDtypeStruct(a.shape, t) for t in types],
        compiler_params=params(16),
        cost_estimate=pl.CostEstimate(flops=5 * 10**8, bytes_accessed=3 << 20, transcendentals=0),
    )(a, b)


def ready_kernel(turn, place, q_ref, g_ref, f_ref, s_ref):
    heads, size = q_ref.shape[2:]
    which = sequence(place, turn)
    queries = pltpu.einshape("thd->htd", q_ref[which])
    gates = pltpu.einshape("thd->htd", g_ref[which])
    for h in range(heads):
        cut = slice(h * size, (h + 1) * size)
        f_ref[:, cut] = feature(queries[h])
        s_ref[:, cut] = 1.0 + jnp.exp(-gates[h].astype(F32))


def ready(place, turn, queries, gates):
    _, tokens, heads, size = queries.shape
    vmem = pl.BlockSpec(memory_space=pltpu.VMEM)
    shape = (tokens, heads * size)
    return pl.pallas_call(
        functools.partial(ready_kernel, turn),
        in_specs=[pl.BlockSpec(memory_space=pltpu.SMEM), vmem, vmem],
        out_specs=[vmem, vmem],
        out_shape=[jax.ShapeDtypeStruct(shape, BF16), jax.ShapeDtypeStruct(shape, F32)],
        compiler_params=params(8),
        cost_estimate=pl.CostEstimate(flops=4 * 10**9, bytes_accessed=10 << 20, transcendentals=0),
        name="ready",
    )(place, queries, gates)


def head_at(place, n):
    y, x, core = place[0] >> 2, place[0] & 3, place[1] & 1
    second, first = OFFSETS[n // SIDE], OFFSETS[n % SIDE]
    down, across = jnp.where(core == 0, second, first), jnp.where(core == 0, first, second)
    return ((y + down) & 3) * SIDE + ((x + across) & 3)


def read_kernel(place, f_ref, s_ref, state_ref, mixed_ref, rhs):
    heads = state_ref.shape[0] - 1
    size = state_ref.shape[-1]
    for h in range(heads):
        rhs[h, :size, :size] = state_ref[h]
        rhs[h, :size, size:] = jnp.zeros((size, size), BF16)
        rhs[h, size:, :size] = jnp.broadcast_to(state_ref[heads, h : h + 1, :], (size, size))
        rhs[h, size:, size:] = jnp.broadcast_to(state_ref[heads, heads + h : heads + h + 1, :], (size, size))
    for n in range(heads):
        h = head_at(place, n)
        cut = pl.ds(pl.multiple_of(h * size, size), size)
        f = f_ref[:, cut]
        both = lax.dot_general(
            jnp.concatenate([f, f], axis=1), rhs[h], (((1,), (1,)), ((), ())), preferred_element_type=F32
        )
        scale = 64.0 / ((both[:, size:] + 1.024) * s_ref[:, cut])
        mixed_ref[:, n * size : (n + 1) * size] = (both[:, :size] * scale).astype(BF16)


def read(place, features, scale, state):
    tokens, width = features.shape
    size = state.shape[-1]
    vmem = pl.BlockSpec(memory_space=pltpu.VMEM)
    return pl.pallas_call(
        read_kernel,
        in_specs=[pl.BlockSpec(memory_space=pltpu.SMEM)] + [vmem] * 3,
        out_specs=vmem,
        out_shape=jax.ShapeDtypeStruct((tokens, width), BF16),
        scratch_shapes=[pltpu.VMEM((width // size, 2 * size, 2 * size), BF16)],
        compiler_params=params(8),
        cost_estimate=pl.CostEstimate(flops=3 * 10**9, bytes_accessed=8 << 20, transcendentals=0),
        name="read",
    )(place, features, scale, state)


def product(mixed_ref, rows, piece_refs, side, total=None):
    size = piece_refs[0][1].shape[1]
    for p, piece in piece_refs:
        slots = [p * SIDE + q if side == 0 else q * SIDE + p for q in range(SIDE)]
        left = jnp.concatenate([mixed_ref[rows, n * size : (n + 1) * size] for n in slots], axis=1)
        part = jnp.dot(left, piece[...].reshape(SIDE * size, -1), preferred_element_type=F32)
        total = part if total is None else total + part
    return total


def open_kernel(numbers, mixed_refs, own_refs, partner_ref, own_out, partner_out):
    block = own_out.shape[1] // pl.num_programs(0)
    rows = pl.ds(pl.multiple_of(pl.program_id(0) * block, block), block)
    for t, mixed in enumerate(mixed_refs):
        own_out[t, rows, :] = product(mixed, rows, list(zip(numbers, own_refs)), 0)
    some = [(p, partner_ref.at[i]) for i, p in enumerate(numbers)]
    partner_out[rows, :] = product(mixed_refs[0], rows, some, 1)


def open_products(mixed, numbers, own, partner):
    vmem = pl.BlockSpec(memory_space=pltpu.VMEM)
    tokens, half = mixed[0].shape[0], partner.shape[-1]
    return pl.pallas_call(
        functools.partial(open_kernel, numbers),
        grid=(2,),
        in_specs=[[vmem] * 2, [vmem] * len(own), vmem],
        out_specs=[vmem] * 2,
        out_shape=[jax.ShapeDtypeStruct((2, tokens, half), F32), jax.ShapeDtypeStruct((tokens, half), F32)],
        compiler_params=params(10),
        cost_estimate=pl.CostEstimate(flops=4 * 10**9, bytes_accessed=8 << 20, transcendentals=0),
        name="open_products",
    )(mixed, own, partner)


def middle_kernel(early, late, mixed_refs, open_ref, late_refs, partner_ref, own_out, partner_out):
    block = own_out.shape[1] // pl.num_programs(0)
    rows = pl.ds(pl.multiple_of(pl.program_id(0) * block, block), block)
    for t, mixed in enumerate(mixed_refs):
        own_out[t, rows, :] = product(mixed, rows, list(zip(late, late_refs)), 0, open_ref[t, rows, :]).astype(BF16)
    some = [(p, partner_ref.at[i]) for i, p in enumerate(early)]
    partner_out[rows, :] = product(mixed_refs[1], rows, some, 1)


def middle_products(mixed, early, late, opened, own, partner):
    vmem = pl.BlockSpec(memory_space=pltpu.VMEM)
    tokens, half = mixed[0].shape[0], partner.shape[-1]
    return pl.pallas_call(
        functools.partial(middle_kernel, early, late),
        grid=(2,),
        in_specs=[[vmem] * 2, vmem, [vmem] * len(own), vmem],
        out_specs=[vmem] * 2,
        out_shape=[jax.ShapeDtypeStruct((2, tokens, half), BF16), jax.ShapeDtypeStruct((tokens, half), F32)],
        compiler_params=params(10),
        cost_estimate=pl.CostEstimate(flops=4 * 10**9, bytes_accessed=8 << 20, transcendentals=0),
        name="middle_products",
    )(mixed, opened, own, partner)


def last_kernel(numbers, place, mixed_refs, open_refs, half_ref, piece_refs, out_ref, held, sems, half_sems):
    cuts, block, half = held.shape
    per = cuts // 2

    def columns(side):
        return pl.ds(pl.multiple_of(sequence(place, side) * half, half), half)

    copies = []
    for t in range(2):
        copies.append(pltpu.make_async_copy(half_ref.at[t], out_ref.at[sequence(place, t), :, columns(0)], half_sems.at[t]))
        copies[-1].start()
    for t, mixed in enumerate(mixed_refs):
        for i in range(per):
            n = t * per + i
            rows = slice(i * block, (i + 1) * block)
            some = [(p, piece_refs.at[j]) for j, p in enumerate(numbers)]
            held[n] = product(mixed, rows, some, 1, open_refs[t][rows, :]).astype(BF16)
            target = out_ref.at[sequence(place, t), pl.ds(i * block, block), columns(1)]
            copies.append(pltpu.make_async_copy(held.at[n], target, sems.at[n]))
            copies[-1].start()
    for copy in copies:
        copy.wait()


def last_half(place, mixed, opened, half, numbers, pieces):
    tokens, width = mixed[0].shape
    block = 256
    vmem = pl.BlockSpec(memory_space=pltpu.VMEM)
    cuts = 2 * tokens // block
    return pl.pallas_call(
        functools.partial(last_kernel, numbers),
        in_specs=[pl.BlockSpec(memory_space=pltpu.SMEM), [vmem] * 2, [vmem] * 2, vmem, vmem],
        out_specs=pl.BlockSpec(memory_space=pltpu.HBM),
        out_shape=jax.ShapeDtypeStruct((2, tokens, width), BF16),
        scratch_shapes=[
            pltpu.VMEM((cuts, block, width // 2), BF16),
            pltpu.SemaphoreType.DMA((cuts,)),
            pltpu.SemaphoreType.DMA((2,)),
        ],
        compiler_params=params(10),
        cost_estimate=pl.CostEstimate(flops=3 * 10**9, bytes_accessed=8 << 20, transcendentals=0),
        name="last_half",
    )(place, mixed, opened, half, pieces)


def take_kernel(place, w_ref, out_ref, sem):
    half = out_ref.shape[1]
    columns = pl.ds(pl.multiple_of(sequence(place, 0) * half, half), half)
    copy = pltpu.make_async_copy(w_ref.at[:, columns], out_ref, sem)
    copy.start()
    copy.wait()


def own_columns(place, weight):
    rows, width = weight.shape
    return pl.pallas_call(
        take_kernel,
        in_specs=[pl.BlockSpec(memory_space=pltpu.SMEM), pl.BlockSpec(memory_space=pltpu.HBM)],
        out_specs=pl.BlockSpec(memory_space=pltpu.VMEM),
        out_shape=jax.ShapeDtypeStruct((rows, width // 2), weight.dtype),
        scratch_shapes=[pltpu.SemaphoreType.DMA],
        compiler_params=params(4),
        cost_estimate=pl.CostEstimate(flops=6 * 10**9, bytes_accessed=1 << 20, transcendentals=0),
        name="own_columns",
    )(place, weight)


def body(queries_in, keys_in, values_in, gate_rows, out_weight):
    outer, span = lax.axis_index("outer"), lax.axis_index("span")
    place = jnp.stack([outer, span]).astype(jnp.int32)
    own = own_columns(place, pltpu.with_memory_space_constraint(out_weight, pltpu.HBM))

    near = [permute(own, shifted(by, True)) for by in (1, -1, 2)]
    stack = jnp.stack([own] + near)
    stacks = [stack] + [permute(stack, shifted(by, False)) for by in (1, -1, 2)]
    early, late = (0, 3), (1, 2)
    swapped = []
    for numbers in (early, late):
        swapped.append(permute(jnp.stack([stacks[p] for p in numbers]), to_partner))

    theirs = local_state(place, 1, keys_in, values_in)
    came = permute(theirs, to_partner)
    own = local_state(place, 0, keys_in, values_in)
    total, send = join(first_kernel, own, came, (F32, F32))
    came = permute(send.astype(F16), along_z(True)).astype(F32)
    total, send = join(next_kernel, total, came, (F32, F32))
    came = permute(send.astype(F16), along_z(False)).astype(F32)
    (done,) = join(next_kernel, total, came, (BF16,))
    other = permute(done, to_partner)
    mixed = []
    for turn, state in enumerate((done, other)):
        features, scale = ready(place, turn, queries_in, gate_rows)
        mixed.append(read(place, features, scale, state))
    own_open, first_open = open_products(mixed, early, [stacks[p] for p in early], swapped[0])
    half, second_open = middle_products(mixed, early, late, own_open, [stacks[p] for p in late], swapped[0])
    return last_half(place, mixed, [first_open, second_open], half, late, swapped[1])


def solution(mesh):
    rows = P("outer", "span", None, None)
    return jax.shard_map(
        lambda *args: body(*args),
        mesh=mesh,
        in_specs=(rows, rows, rows, rows, P("outer", None)),
        out_specs=P("outer", "span", None),
        check_vma=False,
    )
```
